128 devices in a mesh: section: 8 (over x, core), expert: 8 (over z, y_lo), tensor: 2 (over y_hi).
Axes of the slice: x: 4, y: 4 (y_hi: 2, y_lo: 2; y = y_hi * 2 + y_lo), z: 4, core: 2. Of those that a mesh axis runs over, the one named last changes fastest.
Arguments:
- tokens: bfloat16 [2, 8, 1024, 2048], P(None, 'section', ('expert', 'tensor')), may hold values from -26 to 26
- norm_gain: bfloat16 [8, 2048], P('section'), may hold values from 0.099609375 to 1.8984375
- router_weight: bfloat16 [8, 2048, 8], P('section'), may hold values from -0.125 to 0.125
- gate_up: bfloat16 [8, 8, 2048, 5632], P('section', 'expert', None, 'tensor'), may hold values from -0.125 to 0.125
- down_proj: bfloat16 [8, 8, 2816, 2048], P('section', 'expert', 'tensor'), may hold values from -0.109375 to 0.109375
- expert_ids: int32 [2, 2, 8, 1024, 2], P(None, None, 'section', ('expert', 'tensor')), may hold values from 0 to 7, all different within a row; in each aligned block of 64 rows (0 to 63, 64 to 127, ..., all dimensions but the last counted through in order) at most 20 rows name the same one
Outputs:
- blocks_out: bfloat16 [2, 8, 1024, 2048], P(None, 'section', ('expert', 'tensor'))
The draws below stay inside these ranges and needn't reach their ends.
Inputs may be any that keep to these rules, and one draw needn't show every extreme that they name: `expert_ids`: within each aligned block of 64 rows (the rows of one device for one tick, direction and section) no expert is named by more than 20 rows, a bound that some block reaches; the two ids of a row differ.
All inputs are finite; a program needn't handle non-finite values.
Results may differ from the reference program's by a relative error of at most 0.0065.
Values may be sent and summed in bfloat16 or wider, within the bound.
No kernel may reach another device: no remote copies, remote signals or barrier semaphores. Data moves between devices by JAX's collectives and lax.ppermute only.
A program may use at most 128 MiB of HBM per device.

```python
import math
import jax
import jax.numpy as jnp
import numpy as np
from jax import lax

D = 2048
TOP = 2
FF_DEV = 1408
TOK_DEV = 64
TICKS = 2
SECTIONS = 8
EXPERTS = 8
FF = 2816
TOKENS = 1024
CAP = 20
N_TENSOR = 2


def draw_tokens(key, part):
    key_entries = jax.random.fold_in(key, 11)
    key_rows = jax.random.fold_in(key, 12)
    key_cols = jax.random.fold_in(key, 13)
    shape = (2, SECTIONS, TOKENS, D)
    entries = jnp.clip(jax.random.normal(key_entries, shape, jnp.float32), -4.0, 4.0)
    row_scale = jnp.exp(jax.random.uniform(key_rows, (2, SECTIONS, TOKENS, 1), jnp.float32, math.log(0.5), math.log(2.0)))
    col_scale = jnp.exp(jax.random.uniform(key_cols, (1, 1, 1, D), jnp.float32, math.log(0.5), math.log(2.0)))
    values = entries * row_scale * col_scale
    return values.astype(jnp.bfloat16)


def level_of(own_key, dims, shards, low, largest):
    def one(position, blocks):
        steps = jax.random.uniform(jax.random.fold_in(jax.random.fold_in(own_key, 6), position), (blocks,), jnp.float32, low / len(shards), largest / len(shards))
        return jnp.repeat(jnp.exp(steps), dims[position] // blocks).reshape((-1,) + (1,) * (len(dims) - position - 1))

    factor_of = one(*shards[0])
    for cut in shards[1:]:
        factor_of = factor_of * one(*cut)
    return factor_of


def routed_block(own_key, own, number, rows, number_of, top, most, slope):
    order = jax.random.permutation(own_key, number_of)
    packed, usual = portions_of(number_of, rows * top, most, slope, True), portions_of(number_of, rows * top, most, slope, False)
    places = jnp.arange(number_of)

    def named(sizes, rotation):
        used = int((sizes > 0).sum())
        fixed = max(1, used // 4)
        moved = fixed + (places - fixed + rotation * (used - fixed)) % max(1, number_of - fixed)
        return jnp.zeros((number_of,), jnp.int32).at[order[jnp.where(places < fixed, places, moved)]].set(jnp.asarray(sizes, jnp.int32))

    sizes = jnp.where(number % 4 == 0, named(packed, number // 4), named(usual, number - number // 4 - 1))
    mixed = jax.random.permutation(jax.random.fold_in(own, 3), number_of)
    giver, receiver = mixed[0:number_of // 2 * 2:2], mixed[1:number_of // 2 * 2:2]
    slack = jnp.minimum(sizes[giver] - 1, most - sizes[receiver]) // 2
    slack = jnp.where((giver == order[0]) | (receiver == order[0]) | (sizes[receiver] == 0), 0, jnp.maximum(slack, 0))
    moved = jax.random.randint(jax.random.fold_in(own, 4), (number_of // 2,), 0, 1 << 20) % (slack + 1)
    sizes = sizes.at[giver].add(-moved).at[receiver].add(moved)
    items = jnp.searchsorted(jnp.cumsum(sizes), jnp.arange(rows * top), side="right").astype(jnp.int32)
    grid = items.reshape(top, rows).T
    grid = grid[jax.random.permutation(jax.random.fold_in(own, 1), rows)]
    rotation = jax.random.randint(jax.random.fold_in(own, 2), (rows, 1), 0, top)
    return jnp.take_along_axis(grid, (jnp.arange(top)[None, :] + rotation) % top, axis=1)


def portions_of(count, total, reach, lean, full):
    weights = [(1 << 20) // math.isqrt(grade ** lean) + 1 for grade in range(1, count + 1)]
    largest = reach if full else min(reach, max(-(-total // count), total * weights[0] // sum(weights)))
    least = 1 if total - largest >= count - 1 else 0
    given, spare = [largest] + [least] * (count - 1), total - largest - least * (count - 1)
    while spare > 0:
        movable = [i for i in range(1, count) if given[i] < largest] or [i for i in range(1, count) if given[i] < reach]
        whole, budget = sum([weights[i] for i in movable]), spare
        for i in movable:
            addition = min(reach - given[i], max(1, budget * weights[i] // whole), spare)
            given[i] = given[i] + addition
            spare = spare - addition
    return np.array(given)


def normal_values(stream_key, extent, scale, bound, cuts=(), kind=jnp.bfloat16):
    values = jax.random.normal(stream_key, extent, jnp.float32) * scale
    if len(cuts) > 0:
        values = level_of(stream_key, extent, cuts, -0.22, 0.18) * values
    return jnp.clip(values, min=-bound, max=bound).astype(kind)


def setup_inputs(seed: int = 0) -> dict:
    arg_keys = jax.random.split(jax.random.key(seed), 7)
    tokens = draw_tokens(jax.random.fold_in(arg_keys[6], 71), 0)
    norm_gain = jnp.clip(1.0 + 0.18 * jax.random.normal(arg_keys[1], (SECTIONS, D), jnp.float32), 0.099609375, 1.8984375).astype(jnp.bfloat16)
    router_weight = normal_values(arg_keys[2], (SECTIONS, D, EXPERTS), D ** -0.5, 0.125, ((0, 8),))
    gate_up = normal_values(arg_keys[3], (SECTIONS, EXPERTS, D, 2 * FF), D ** -0.5, 0.125, ((0, 8), (1, 8), (3, 2)))
    down_proj = normal_values(arg_keys[4], (SECTIONS, EXPERTS, FF, D), FF ** -0.5, 0.109375, ((0, 8), (1, 8), (2, 2)))
    expert_ids_keys = jax.random.split(jax.random.fold_in(arg_keys[5], 1), TICKS * 2 * SECTIONS * TOKENS // TOK_DEV)
    expert_ids_turns = jax.random.permutation(jax.random.fold_in(arg_keys[5], 3), TICKS * 2 * SECTIONS * TOKENS // TOK_DEV)
    expert_ids = jax.vmap(lambda own, number: routed_block(jax.random.fold_in(arg_keys[5], 2), own, number, TOK_DEV, EXPERTS, TOP, CAP, 2))(expert_ids_keys, expert_ids_turns).reshape((TICKS, 2, SECTIONS, TOKENS, TOP))
    return {"tokens": tokens, "norm_gain": norm_gain, "router_weight": router_weight, "gate_up": gate_up, "down_proj": down_proj, "expert_ids": expert_ids}


EPSILON = 1e-05

def slot_positions(expert_ids, experts, capacity):
    leading, row_count, picked = expert_ids.shape
    flat_ids = expert_ids.reshape(leading, row_count * picked)
    onehot = (flat_ids[:, :, None] == jnp.arange(experts, dtype=jnp.int32)[None, None, :]).astype(jnp.int32)
    running = jnp.cumsum(onehot, axis=1) - 1
    slot_index = lax.optimization_barrier(jnp.sum(running * onehot, axis=2)).astype(jnp.int32)
    return (flat_ids * capacity + slot_index).astype(jnp.int32).reshape(leading, row_count, picked)

def prepare(blocks, gain_row, router, expert_ids, experts, capacity):
    leading, row_count, width = blocks.shape
    values = blocks.astype(jnp.float32)
    scale = lax.rsqrt(lax.optimization_barrier(jnp.mean(values * values, axis=-1, keepdims=True)) + EPSILON)
    normed = (values * scale * gain_row.astype(jnp.float32)).astype(jnp.bfloat16)
    logits = jnp.dot(normed.reshape(-1, width), router, preferred_element_type=jnp.float32)
    logits = logits.reshape(leading, row_count, experts)
    selector = expert_ids[..., None] == jnp.arange(experts, dtype=jnp.int32)
    chosen = lax.optimization_barrier(jnp.sum(jnp.where(selector, logits[:, :, None, :], jnp.float32(0.0)), axis=-1))
    first = jax.nn.sigmoid(chosen[..., 0] - chosen[..., 1])
    second = jax.nn.sigmoid(chosen[..., 1] - chosen[..., 0])
    weights = jnp.stack([first, second], axis=-1)
    positions = slot_positions(expert_ids, experts, capacity)
    table = positions[:, None, :, :] == jnp.arange(experts * capacity, dtype=jnp.int32)[None, :, None, None]
    dispatch = lax.optimization_barrier(jnp.sum(table.astype(jnp.float32), axis=-1))
    routed = jnp.einsum('bpr,brd->bpd', dispatch, normed.astype(jnp.float32)).astype(jnp.bfloat16)
    return (weights, positions, routed)

def combine(blocks, results, weights, positions):
    leading, row_count, width = blocks.shape
    picked = jax.vmap(lambda table_rows, index: table_rows[index])(results, positions.reshape(leading, -1))
    picked = picked.reshape(leading, row_count, 2, width).astype(jnp.float32)
    total = blocks.astype(jnp.float32) + lax.optimization_barrier(jnp.sum(weights[..., None] * picked, axis=2))
    return total.astype(jnp.bfloat16)

def layer(block_rows, gain_row, router, combined_all, down_all, ids):
    blocks_count = TOKENS // TOK_DEV
    grouped = block_rows.reshape(blocks_count, TOK_DEV, D)
    ids_grouped = ids.reshape(blocks_count, TOK_DEV, TOP)
    weights, positions, routed = prepare(grouped, gain_row, router, ids_grouped, EXPERTS, CAP)
    routed = routed.reshape(blocks_count, EXPERTS, CAP, D)

    def one_expert(operands):
        rows_in, combined, down = operands
        flat = rows_in.reshape(-1, D)
        gate_part = jnp.dot(flat, combined[:, :FF], preferred_element_type=jnp.float32).astype(jnp.bfloat16)
        up_part = jnp.dot(flat, combined[:, FF:], preferred_element_type=jnp.float32).astype(jnp.bfloat16)
        gate_part, up_part = lax.optimization_barrier((gate_part, up_part))
        hidden = (jax.nn.silu(gate_part.astype(jnp.float32)) * up_part.astype(jnp.float32)).astype(jnp.bfloat16)
        total = jnp.zeros((flat.shape[0], D), jnp.float32)
        for half_index in range(N_TENSOR):
            start = half_index * FF_DEV
            piece = jnp.dot(hidden[:, start:start + FF_DEV], down[start:start + FF_DEV], preferred_element_type=jnp.float32)
            piece = lax.optimization_barrier(piece.astype(jnp.bfloat16))
            total = total + piece.astype(jnp.float32)
        result = lax.optimization_barrier(total.astype(jnp.bfloat16))
        return result.reshape(blocks_count, CAP, D)
    results = lax.map(one_expert, (jnp.moveaxis(routed, 1, 0), combined_all, down_all))
    results = jnp.moveaxis(results, 0, 1).reshape(blocks_count, EXPERTS * CAP, D)
    return combine(grouped, results, weights, positions).reshape(TOKENS, D)

def reference(tokens, norm_gain, router_weight, gate_up, down_proj, expert_ids):
    state = tokens
    for tick_index in range(TICKS):
        outputs = []
        for direction in range(2):
            per_section = []
            for section_index in range(SECTIONS):
                per_section.append(layer(state[direction, section_index], norm_gain[section_index], router_weight[section_index], gate_up[section_index], down_proj[section_index], expert_ids[tick_index, direction, section_index]))
            outputs.append(jnp.stack(per_section))
        forward = jnp.roll(outputs[0], 1, axis=0)
        backward = jnp.roll(outputs[1], -1, axis=0)
        state = jnp.stack([forward, backward])
    return state
```

```python
import functools

import jax
import jax.numpy as jnp
from jax import lax
from jax.experimental import pallas as pl
from jax.experimental.pallas import tpu as pltpu
from jax.sharding import PartitionSpec as P

TICKS = 2
EPSILON = 1e-05

BF16 = jnp.bfloat16
F32 = jnp.float32
VMEM = pl.BlockSpec(memory_space=pltpu.VMEM)
SMEM = pl.BlockSpec(memory_space=pltpu.SMEM)
ANY = pl.BlockSpec(memory_space=pl.ANY)

Z = 4
Y = 4
AXES = ("section", "expert", "tensor")
PLANE = ("expert", "tensor")


def plane_index(z, y):
    return (z * 2 + y % 2) * 2 + y // 2


def y_shift(array, by):
    pairs = [
        (plane_index(z, y), plane_index(z, (y + by) % Y)) for z in range(Z) for y in range(Y)
    ]
    return lax.ppermute(array, PLANE, pairs)


def z_shift(array, by):
    pairs = [
        (plane_index(z, y), plane_index((z + by) % Z, y)) for z in range(Z) for y in range(Y)
    ]
    return lax.ppermute(array, PLANE, pairs)


def section_shift(array, by, y_by):
    sections = lax.axis_size("section")
    plane = Z * Y
    pairs = [
        (
            s * plane + plane_index(z, y),
            (s + by) % sections * plane + plane_index(z, (y + y_by) % Y),
        )
        for s in range(sections)
        for z in range(Z)
        for y in range(Y)
    ]
    return lax.ppermute(array, AXES, pairs)


def from_partner(array):
    return lax.ppermute(array, "tensor", [(0, 1), (1, 0)])


def shape(rows, columns, dtype=BF16):
    return jax.ShapeDtypeStruct((rows, columns), dtype)


def params(limit_mib):
    return pltpu.CompilerParams(vmem_limit_bytes=limit_mib * 1024 * 1024)


def cost(flops, bytes_accessed):
    return pl.CostEstimate(
        flops=int(flops), bytes_accessed=int(bytes_accessed), transcendentals=0
    )


def norm_body(count, *refs):
    parts, gain_ref, outs = refs[:count], refs[count], refs[count + 1 :]
    values = parts[0][...].astype(F32)
    if count > 1:
        for part in parts[1:]:
            values = values + part[...].astype(F32)
        state = values.astype(BF16)
        outs[0][...] = state
        values = state.astype(F32)
    scale = lax.rsqrt(jnp.mean(values * values, axis=-1, keepdims=True) + EPSILON)
    outs[-1][...] = (values * scale * gain_ref[...].astype(F32)).astype(BF16)


def norm(parts, gain):
    rows, width = parts[0].shape
    count = len(parts)
    outs = [shape(rows, width)] * (2 if count > 1 else 1)
    return pl.pallas_call(
        functools.partial(norm_body, count),
        out_shape=outs,
        in_specs=[VMEM] * (count + 1),
        out_specs=[VMEM] * len(outs),
        compiler_params=params(12),
        cost_estimate=cost(2e8, (count + 2) * rows * width * 2),
        name="norm",
    )(*parts, gain)


def slots_body(capacity, place_ref, ids_ref, *refs):
    blocks, outs = refs[:Y], refs[Y:]
    my_z, my_low, half = place_ref[0], place_ref[1], place_ref[2]
    rows = blocks[0].shape[0]
    total = rows * Y
    per = capacity * Y
    expert = lax.broadcasted_iota(jnp.int32, (8, total), 0)
    row = lax.broadcasted_iota(jnp.int32, (8, total), 1)
    first, second = ids_ref[0:1, :], ids_ref[1:2, :]
    named = jnp.where((expert == first) | (expert == second), 1.0, 0.0).astype(BF16)
    a = lax.broadcasted_iota(jnp.int32, (total, total), 0)
    b = lax.broadcasted_iota(jnp.int32, (total, total), 1)
    earlier = jnp.where((a < b) & (a // rows == b // rows), 1.0, 0.0).astype(BF16)
    position = jnp.dot(named, earlier, preferred_element_type=F32).astype(jnp.int32)
    step = (expert // 2 - my_z + Z) % Z
    block = (row // rows + 2 * half) % Y
    slot = jnp.where(
        expert % 2 == my_low, step * per + block * capacity + position, -1
    )
    slot0 = jnp.max(jnp.where(expert == first, slot, -1), axis=0, keepdims=True)
    slot1 = jnp.max(jnp.where(expert == second, slot, -1), axis=0, keepdims=True)
    target = lax.broadcasted_iota(jnp.int32, (per * Z, total), 0)
    chosen = jnp.where((target == slot0) | (target == slot1), 1.0, 0.0).astype(BF16)
    everything = jnp.concatenate([block[...] for block in blocks], axis=0)
    placed = jnp.dot(chosen, everything, preferred_element_type=F32).astype(BF16)
    for k in range(Z):
        outs[k][...] = placed[k * per : (k + 1) * per]


def fill_slots(place, ids_rows, blocks, capacity):
    rows, width = blocks[0].shape
    per = capacity * Y
    return pl.pallas_call(
        functools.partial(slots_body, capacity),
        out_shape=[shape(per, width)] * Z,
        in_specs=[SMEM, VMEM] + [VMEM] * Y,
        out_specs=[VMEM] * Z,
        compiler_params=params(16),
        cost_estimate=cost(1e9, 8 * per * width * 2),
        name="slots",
    )(place, ids_rows, *blocks)


def weights_body(capacity, place_ref, ids_ref, router_ref, *refs):
    blocks, (high_ref, low_ref) = refs[:Y], refs[Y:]
    my_z, my_low, half = place_ref[0], place_ref[1], place_ref[2]
    rows = blocks[0].shape[0]
    total = rows * Y
    per = capacity * Y
    experts = router_ref.shape[1]
    everything = jnp.concatenate([block[...] for block in blocks], axis=0)
    logits = jnp.dot(everything, router_ref[...], preferred_element_type=F32)
    first, second = ids_ref[:, 0:1], ids_ref[:, 1:2]
    expert = lax.broadcasted_iota(jnp.int32, (total, experts), 1)
    row = lax.broadcasted_iota(jnp.int32, (total, experts), 0)
    at0, at1 = expert == first, expert == second
    named = jnp.where(at0 | at1, 1.0, 0.0).astype(BF16)
    a = lax.broadcasted_iota(jnp.int32, (total, total), 0)
    b = lax.broadcasted_iota(jnp.int32, (total, total), 1)
    earlier = jnp.where((b < a) & (a // rows == b // rows), 1.0, 0.0).astype(BF16)
    position = jnp.dot(earlier, named, preferred_element_type=F32).astype(jnp.int32)
    step = (expert // 2 - my_z + Z) % Z
    block = (row // rows + 2 * half) % Y
    slot = jnp.where(
        expert % 2 == my_low, step * per + block * capacity + position, -1
    )
    slot0 = jnp.max(jnp.where(at0, slot, -1), axis=1, keepdims=True)
    slot1 = jnp.max(jnp.where(at1, slot, -1), axis=1, keepdims=True)
    one = jnp.sum(jnp.where(at0, logits, 0.0), axis=1, keepdims=True)
    two = jnp.sum(jnp.where(at1, logits, 0.0), axis=1, keepdims=True)
    weight0 = 1.0 / (1.0 + jnp.exp(two - one))
    weight1 = 1.0 / (1.0 + jnp.exp(one - two))
    target = lax.broadcasted_iota(jnp.int32, (total, per * Z), 1)
    spread = jnp.where(target == slot0, weight0, jnp.where(target == slot1, weight1, 0.0))
    high = spread.astype(BF16)
    high_ref[...] = high
    low_ref[...] = (spread - high.astype(F32)).astype(BF16)


def spread_weights(place, ids_columns, router, blocks, capacity):
    rows, width = blocks[0].shape
    per = capacity * Y
    return pl.pallas_call(
        functools.partial(weights_body, capacity),
        out_shape=[shape(rows * Y, per * Z)] * 2,
        in_specs=[SMEM, VMEM, VMEM] + [VMEM] * Y,
        out_specs=[VMEM] * 2,
        compiler_params=params(16),
        cost_estimate=cost(1e9, 2e6),
        name="weights",
    )(place, ids_columns, router, *blocks)


def product_body(steps, flip, place_ref, weight_ref, *refs):
    slots, out_ref, held, rows_ref, sems = refs[:Z], refs[Z], refs[Z + 1], refs[Z + 2], refs[Z + 3]
    half = place_ref[2]
    if flip:
        half = 1 - half
    depth, units = held.shape[1], held.shape[2]
    start = pl.multiple_of(half * units, 128)
    copies = [
        pltpu.make_async_copy(
            weight_ref.at[pl.ds(i * depth, depth), pl.ds(start, units)],
            held.at[i],
            sems.at[i],
        )
        for i in range(steps)
    ]
    for copy in copies:
        copy.start()
    per = slots[0].shape[0]
    for k in range(Z):
        rows_ref[k * per : (k + 1) * per, :] = slots[k][...]
    total = None
    for i in range(steps):
        copies[i].wait()
        part = jnp.dot(
            rows_ref[:, i * depth : (i + 1) * depth], held[i], preferred_element_type=F32
        )
        total = part if total is None else total + part
    out_ref[...] = total.astype(BF16)


def product(place, combined, slots, flip):
    per, width = slots[0].shape
    units = combined.shape[1] // 2
    steps = 4
    return pl.pallas_call(
        functools.partial(product_body, steps, flip),
        out_shape=shape(per * Z, units),
        in_specs=[SMEM, ANY] + [VMEM] * Z,
        out_specs=VMEM,
        scratch_shapes=[
            pltpu.VMEM((steps, width // steps, units), BF16),
            pltpu.VMEM((per * Z, width), BF16),
            pltpu.SemaphoreType.DMA((steps,)),
        ],
        compiler_params=params(24),
        cost_estimate=cost(2 * per * Z * width * units, width * units * 2),
        name="product_other" if flip else "product_own",
    )(place, combined, *slots)


def down_body(steps, place_ref, own_ref, partner_ref, weight_ref, *refs):
    outs, held, hidden_ref, sems = refs[:Z], refs[Z], refs[Z + 1], refs[Z + 2]
    columns = held.shape[2]
    copies = [
        pltpu.make_async_copy(
            weight_ref.at[:, pl.ds(i * columns, columns)], held.at[i], sems.at[i]
        )
        for i in range(steps)
    ]
    for copy in copies:
        copy.start()
    first = place_ref[2] == 0
    own = own_ref[...].astype(F32)
    partner = partner_ref[...].astype(F32)
    gate = jnp.where(first, own, partner)
    up = jnp.where(first, partner, own)
    hidden_ref[...] = (gate / (1.0 + jnp.exp(-gate)) * up).astype(BF16)
    per = outs[0].shape[0]
    for i in range(steps):
        copies[i].wait()
        part = jnp.dot(hidden_ref[...], held[i], preferred_element_type=F32).astype(BF16)
        for k in range(Z):
            outs[k][:, i * columns : (i + 1) * columns] = part[k * per : (k + 1) * per]


def down(place, own, partner, weight):
    rows, units = own.shape
    width = weight.shape[1]
    steps = 4
    per = rows // Z
    return pl.pallas_call(
        functools.partial(down_body, steps),
        out_shape=[shape(per, width)] * Z,
        in_specs=[SMEM, VMEM, VMEM, ANY],
        out_specs=[VMEM] * Z,
        scratch_shapes=[
            pltpu.VMEM((steps, units, width // steps), BF16),
            pltpu.VMEM((rows, units), BF16),
            pltpu.SemaphoreType.DMA((steps,)),
        ],
        compiler_params=params(24),
        cost_estimate=cost(2 * rows * width * units, width * units * 2),
        name="down",
    )(place, own, partner, weight)


def collect_body(high_ref, low_ref, *refs):
    returned, outs = refs[:Z], refs[Z:]
    slots = jnp.concatenate([piece[...] for piece in returned], axis=0)
    total = jnp.dot(high_ref[...], slots, preferred_element_type=F32)
    total = total + jnp.dot(low_ref[...], slots, preferred_element_type=F32)
    total = total.astype(BF16)
    rows = outs[0].shape[0]
    for j in range(Y):
        outs[j][...] = total[j * rows : (j + 1) * rows]


def collect(high, low, returned):
    rows = high.shape[0] // Y
    width = returned[0].shape[1]
    return pl.pallas_call(
        collect_body,
        out_shape=[shape(rows, width)] * Y,
        in_specs=[VMEM] * (2 + Z),
        out_specs=[VMEM] * Y,
        compiler_params=params(16),
        cost_estimate=cost(1e9, 4e6),
        name="collect",
    )(high, low, *returned)


def on_device(tokens, norm_gain, router_weight, gate_up, down_proj, expert_ids):
    experts = router_weight.shape[2]
    rows = tokens.shape[2]
    capacity = rows * 2 * 5 // (4 * experts)
    expert_index = lax.axis_index("expert")
    place = jnp.stack([expert_index // 2, expert_index % 2, lax.axis_index("tensor")]).astype(
        jnp.int32
    )
    combined, down_rows, router = gate_up[0, 0], down_proj[0, 0], router_weight[0]

    ids = expert_ids[:, :, 0].reshape(-1, 128)
    gathered = jnp.stack([ids] + [y_shift(ids, j) for j in range(1, Y)])
    gathered = gathered.reshape(Y, TICKS, 2, rows, 2).transpose(1, 2, 0, 3, 4)
    columns = gathered.reshape(TICKS, 2, Y * rows, 2)
    across = columns.transpose(0, 1, 3, 2)

    parts = [[tokens[0, 0]], [tokens[1, 0]]]
    for tick in range(TICKS):
        streams = []
        for m in (0, 1):
            to_next = 1 if m == 0 else -1
            if tick == 0:
                state = parts[m][0]
                (normed,) = norm(parts[m], norm_gain)
            else:
                state, normed = norm(parts[m], norm_gain)
            blocks = [normed] + [y_shift(normed, j) for j in range(1, Y)]
            slots = fill_slots(place, across[tick, m], blocks, capacity)
            arrived = [slots[0]] + [z_shift(slots[k], k) for k in range(1, Z)]
            other = product(place, combined, arrived, True)
            partner = from_partner(other)
            own = product(place, combined, arrived, False)
            high, low = spread_weights(place, columns[tick, m], router, blocks, capacity)
            back = down(place, own, partner, down_rows)
            returned = [back[0]] + [z_shift(back[k], -k) for k in range(1, Z)]
            sums = collect(high, low, returned)
            residual = section_shift(state, to_next, 0)
            streams.append(
                [residual] + [section_shift(sums[j], to_next, -j) for j in range(Y)]
            )
        parts = streams
    total = [sum(piece.astype(F32) for piece in stream).astype(BF16) for stream in parts]
    return jnp.stack(total)[:, None]


def solution(mesh):
    in_specs = (
        P(None, "section", ("expert", "tensor"), None),
        P("section", None),
        P("section", None, None),
        P("section", "expert", None, "tensor"),
        P("section", "expert", "tensor", None),
        P(None, None, "section", ("expert", "tensor"), None),
    )
    out_specs = P(None, "section", ("expert", "tensor"), None)
    return jax.shard_map(
        on_device, mesh=mesh, in_specs=in_specs, out_specs=out_specs, check_vma=False
    )
```

```python
import functools

import jax
import jax.numpy as jnp
from jax import lax
from jax.experimental import pallas as pl
from jax.experimental.pallas import tpu as pltpu
from jax.sharding import PartitionSpec as P

TICKS = 2
EPSILON = 1e-05

BF16 = jnp.bfloat16
F32 = jnp.float32
VMEM = pl.BlockSpec(memory_space=pltpu.VMEM)
SMEM = pl.BlockSpec(memory_space=pltpu.SMEM)

Z = 4
Y = 4
AXES = ("section", "expert", "tensor")
PLANE = ("expert", "tensor")


def plane_index(z, y):
    return (z * 2 + y % 2) * 2 + y // 2


def y_shift(array, by):
    pairs = [
        (plane_index(z, y), plane_index(z, (y + by) % Y)) for z in range(Z) for y in range(Y)
    ]
    return lax.ppermute(array, PLANE, pairs)


def z_shift(array, by):
    pairs = [
        (plane_index(z, y), plane_index((z + by) % Z, y)) for z in range(Z) for y in range(Y)
    ]
    return lax.ppermute(array, PLANE, pairs)


def section_shift(array, by, y_by):
    sections = lax.axis_size("section")
    plane = Z * Y
    pairs = [
        (
            s * plane + plane_index(z, y),
            (s + by) % sections * plane + plane_index(z, (y + y_by) % Y),
        )
        for s in range(sections)
        for z in range(Z)
        for y in range(Y)
    ]
    return lax.ppermute(array, AXES, pairs)


def from_partner(array):
    return lax.ppermute(array, "tensor", [(0, 1), (1, 0)])


def shape(rows, columns, dtype=BF16):
    return jax.ShapeDtypeStruct((rows, columns), dtype)


def params(limit_mib):
    return pltpu.CompilerParams(vmem_limit_bytes=limit_mib * 1024 * 1024)


def cost(flops, bytes_accessed):
    return pl.CostEstimate(
        flops=int(flops), bytes_accessed=int(bytes_accessed), transcendentals=0
    )


def norm_body(count, *refs):
    parts, gain_ref, (state_ref, out_ref) = refs[:count], refs[count], refs[count + 1 :]
    width = out_ref.shape[1]
    values = parts[0][...].reshape(-1, width).astype(F32)
    for part in parts[1:]:
        values = values + part[...].astype(F32)
    state = values.astype(BF16)
    state_ref[...] = state
    values = state.astype(F32)
    scale = lax.rsqrt(jnp.mean(values * values, axis=-1, keepdims=True) + EPSILON)
    out_ref[...] = (values * scale * gain_ref[...].astype(F32)).astype(BF16)


def norm(parts, gain, index=None):
    rows, width = parts[0].shape[-2:]
    count = len(parts)
    in_specs, extra = [VMEM] * (count + 1), {}
    if index is not None:
        in_specs = [pl.BlockSpec((1, 1, rows, width), lambda i: (index, 0, 0, 0))]
        in_specs.append(pl.BlockSpec((1, width), lambda i: (0, 0)))
        out_spec = pl.BlockSpec((rows, width), lambda i: (0, 0))
        extra = {"grid": (1,)}
    else:
        out_spec = VMEM
    return pl.pallas_call(
        functools.partial(norm_body, count),
        out_shape=[shape(rows, width)] * 2,
        in_specs=in_specs,
        out_specs=[out_spec] * 2,
        compiler_params=params(4),
        cost_estimate=cost(2e8, (count + 2) * rows * width * 2),
        name="norm",
        **extra,
    )(*parts, gain)


def slots_body(pair, capacity, place_ref, router_ref, *refs):
    ids_refs, blocks = refs[:Y], refs[Y : 2 * Y]
    outs, (high_ref, low_ref) = refs[2 * Y : 2 * Y + Z], refs[2 * Y + Z :]
    my_z, my_low, half = place_ref[0], place_ref[1], place_ref[2]
    rows, width = blocks[0].shape
    total = rows * Y
    per = capacity * Y
    experts = router_ref.shape[0]

    logits = jnp.zeros((experts, total), F32)
    for at in range(0, width, 512):
        piece = jnp.concatenate([block[:, at : at + 512] for block in blocks], axis=0)
        logits = logits + lax.dot_general(
            router_ref[:, at : at + 512],
            piece,
            (((1,), (1,)), ((), ())),
            preferred_element_type=F32,
        )

    ids = jnp.concatenate([ref[...] for ref in ids_refs], axis=1)
    first, second = ids[2 * pair : 2 * pair + 1, :], ids[2 * pair + 1 : 2 * pair + 2, :]
    expert = lax.broadcasted_iota(jnp.int32, (experts, total), 0)
    row = lax.broadcasted_iota(jnp.int32, (experts, total), 1)
    at0, at1 = expert == first, expert == second
    named = jnp.where(at0 | at1, 1.0, 0.0).astype(BF16)
    a = lax.broadcasted_iota(jnp.int32, (total, total), 0)
    b = lax.broadcasted_iota(jnp.int32, (total, total), 1)
    earlier = jnp.where((a < b) & (a // rows == b // rows), 1.0, 0.0).astype(BF16)
    position = jnp.dot(named, earlier, preferred_element_type=F32).astype(jnp.int32)
    step = (expert // 2 - my_z + Z) % Z
    block = (row // rows + 2 * half) % Y
    slot = jnp.where(expert % 2 == my_low, step * per + block * capacity + position, -1)
    slot0 = jnp.max(jnp.where(at0, slot, -1), axis=0, keepdims=True)
    slot1 = jnp.max(jnp.where(at1, slot, -1), axis=0, keepdims=True)
    target = lax.broadcasted_iota(jnp.int32, (per * Z, total), 0)
    chosen = jnp.where((target == slot0) | (target == slot1), 1.0, 0.0).astype(BF16)

    @pl.loop(0, width // 512)
    def _(i):
        at = pl.ds(pl.multiple_of(i * 512, 512), 512)
        piece = jnp.concatenate([block[:, at] for block in blocks], axis=0)
        placed = jnp.dot(chosen, piece, preferred_element_type=F32).astype(BF16)
        for k in range(Z):
            outs[k][:, at] = placed[k * per : (k + 1) * per]

    one = jnp.sum(jnp.where(at0, logits, 0.0), axis=0, keepdims=True)
    two = jnp.sum(jnp.where(at1, logits, 0.0), axis=0, keepdims=True)
    weight0 = 1.0 / (1.0 + jnp.exp(two - one))
    weight1 = 1.0 / (1.0 + jnp.exp(one - two))
    spread = jnp.where(target == slot0, weight0, jnp.where(target == slot1, weight1, 0.0))
    high = spread.astype(BF16)
    high_ref[...] = high
    low_ref[...] = (spread - high.astype(F32)).astype(BF16)


def fill_slots(pair, place, router, ids, blocks, capacity):
    rows, width = blocks[0].shape
    per = capacity * Y
    out = pl.pallas_call(
        functools.partial(slots_body, pair, capacity),
        out_shape=[shape(per, width)] * Z + [shape(per * Z, rows * Y)] * 2,
        in_specs=[SMEM, VMEM] + [VMEM] * (2 * Y),
        out_specs=[VMEM] * (Z + 2),
        compiler_params=params(4),
        cost_estimate=cost(1e9, 8 * per * width * 2),
        name="slots",
    )(place, router, *ids, *blocks)
    return out[:Z], out[Z:]


def product_body(flip, place_ref, weight_ref, *refs):
    slots, (out_ref, rows_ref) = refs[:Z], refs[Z:]
    half = place_ref[2]
    if flip:
        half = 1 - half
    units = out_ref.shape[1]
    per = slots[0].shape[0]
    for k in range(Z):
        rows_ref[k * per : (k + 1) * per, :] = slots[k][...]

    def columns(at, count):
        here = pl.ds(pl.multiple_of(half * units + at, 128), count)
        part = jnp.dot(rows_ref[...], weight_ref[:, here], preferred_element_type=F32)
        out_ref[:, pl.ds(pl.multiple_of(at, 128), count)] = part.astype(BF16)

    @pl.loop(0, units // CHUNK)
    def _(i):
        columns(i * CHUNK, CHUNK)

    if units % CHUNK:
        columns(units // CHUNK * CHUNK, units % CHUNK)


CHUNK = 512


def product(place, combined, slots, flip):
    per, width = slots[0].shape
    units = combined.shape[1] // 2
    return pl.pallas_call(
        functools.partial(product_body, flip),
        out_shape=shape(per * Z, units),
        in_specs=[SMEM, VMEM] + [VMEM] * Z,
        out_specs=VMEM,
        scratch_shapes=[pltpu.VMEM((per * Z, width), BF16)],
        compiler_params=params(6),
        cost_estimate=cost(2 * per * Z * width * units, width * units * 2),
        name="product_other" if flip else "product_own",
    )(place, combined, *slots)


def down_body(place_ref, own_ref, partner_ref, weight_ref, *refs):
    outs, hidden_ref = refs[:Z], refs[Z]
    first = place_ref[2] == 0
    rows = own_ref.shape[0]
    width = weight_ref.shape[1]
    band = 32

    @pl.loop(0, rows // band)
    def _(i):
        at = pl.ds(pl.multiple_of(i * band, band), band)
        own = own_ref[at, :].astype(F32)
        partner = partner_ref[at, :].astype(F32)
        gate = jnp.where(first, own, partner)
        up = jnp.where(first, partner, own)
        hidden_ref[at, :] = (gate / (1.0 + jnp.exp(-gate)) * up).astype(BF16)

    per = outs[0].shape[0]

    @pl.loop(0, width // 512)
    def _(i):
        at = pl.ds(pl.multiple_of(i * 512, 512), 512)
        part = jnp.dot(hidden_ref[...], weight_ref[:, at], preferred_element_type=F32)
        part = part.astype(BF16)
        for k in range(Z):
            outs[k][:, at] = part[k * per : (k + 1) * per]


def down(place, own, partner, weight):
    rows, units = own.shape
    width = weight.shape[1]
    per = rows // Z
    return pl.pallas_call(
        down_body,
        out_shape=[shape(per, width)] * Z,
        in_specs=[SMEM, VMEM, VMEM, VMEM],
        out_specs=[VMEM] * Z,
        scratch_shapes=[pltpu.VMEM((rows, units), BF16)],
        compiler_params=params(6),
        cost_estimate=cost(2 * rows * width * units, width * units * 2),
        name="down",
    )(place, own, partner, weight)


def collect_body(high_ref, low_ref, *refs):
    returned, outs = refs[:Z], refs[Z:]
    rows, width = outs[0].shape

    def weighted(weights, piece):
        return lax.dot_general(
            weights, piece, (((0,), (0,)), ((), ())), preferred_element_type=F32
        )

    @pl.loop(0, width // 512)
    def _(i):
        at = pl.ds(pl.multiple_of(i * 512, 512), 512)
        piece = jnp.concatenate([part[:, at] for part in returned], axis=0)
        total = weighted(high_ref[...], piece) + weighted(low_ref[...], piece)
        total = total.astype(BF16)
        for j in range(Y):
            outs[j][:, at] = total[j * rows : (j + 1) * rows]


def collect(high, low, returned):
    rows = high.shape[1] // Y
    width = returned[0].shape[1]
    return pl.pallas_call(
        collect_body,
        out_shape=[shape(rows, width)] * Y,
        in_specs=[VMEM] * (2 + Z),
        out_specs=[VMEM] * Y,
        compiler_params=params(6),
        cost_estimate=cost(1e9, 4e6),
        name="collect",
    )(high, low, *returned)


def on_device(tokens, norm_gain, router_weight, gate_up, down_proj, expert_ids):
    experts = router_weight.shape[2]
    rows = tokens.shape[2]
    capacity = rows * 2 * 5 // (4 * experts)
    expert_index = lax.axis_index("expert")
    place = jnp.stack([expert_index // 2, expert_index % 2, lax.axis_index("tensor")]).astype(
        jnp.int32
    )
    combined, down_rows = gate_up[0, 0], down_proj[0, 0]

    router = router_weight[0].T
    ids = expert_ids[:, :, 0].transpose(0, 1, 3, 2).reshape(-1, rows)
    normed_first = [norm([tokens], norm_gain, m) for m in (0, 1)]
    ids, normed_first[1] = lax.optimization_barrier((ids, normed_first[1]))
    ids = [ids] + [y_shift(ids, j) for j in range(1, Y)]

    parts = None
    for tick in range(TICKS):
        streams = []
        for m in (0, 1):
            to_next = 1 if m == 0 else -1
            state, normed = normed_first[m] if tick == 0 else norm(parts[m], norm_gain)
            blocks = [normed] + [y_shift(normed, j) for j in range(1, Y)]
            slots, (high, low) = fill_slots(2 * tick + m, place, router, ids, blocks, capacity)
            arrived = [slots[0]] + [z_shift(slots[k], k) for k in range(1, Z)]
            other = product(place, combined, arrived, True)
            partner = from_partner(other)
            own = product(place, combined, arrived, False)
            back = down(place, own, partner, down_rows)
            returned = [back[0]] + [z_shift(back[k], -k) for k in range(1, Z)]
            sums = collect(high, low, returned)
            residual = section_shift(state, to_next, 0)
            streams.append(
                [residual] + [section_shift(sums[j], to_next, -j) for j in range(Y)]
            )
        parts = streams
    total = [sum(piece.astype(F32) for piece in stream).astype(BF16) for stream in parts]
    return jnp.stack(total)[:, None]


def solution(mesh):
    in_specs = (
        P(None, "section", ("expert", "tensor"), None),
        P("section", None),
        P("section", None, None),
        P("section", "expert", None, "tensor"),
        P("section", "expert", "tensor", None),
        P(None, None, "section", ("expert", "tensor"), None),
    )
    out_specs = P(None, "section", ("expert", "tensor"), None)
    return jax.shard_map(
        on_device, mesh=mesh, in_specs=in_specs, out_specs=out_specs, check_vma=False
    )
```

```python
import functools

import jax
import jax.numpy as jnp
from jax import lax
from jax.experimental import pallas as pl
from jax.experimental.pallas import tpu as pltpu
from jax.sharding import PartitionSpec as P

TICKS = 2
EPSILON = 1e-05

BF16 = jnp.bfloat16
F32 = jnp.float32
VMEM = pl.BlockSpec(memory_space=pltpu.VMEM)
SMEM = pl.BlockSpec(memory_space=pltpu.SMEM)

Z = 4
Y = 4
AXES = ("section", "expert", "tensor")
PLANE = ("expert", "tensor")


def plane_index(z, y):
    return (z * 2 + y % 2) * 2 + y // 2


def y_shift(array, by):
    pairs = [
        (plane_index(z, y), plane_index(z, (y + by) % Y)) for z in range(Z) for y in range(Y)
    ]
    return lax.ppermute(array, PLANE, pairs)


def z_shift(array, by):
    pairs = [
        (plane_index(z, y), plane_index((z + by) % Z, y)) for z in range(Z) for y in range(Y)
    ]
    return lax.ppermute(array, PLANE, pairs)


def section_shift(array, by, y_by):
    sections = lax.axis_size("section")
    plane = Z * Y
    pairs = [
        (
            s * plane + plane_index(z, y),
            (s + by) % sections * plane + plane_index(z, (y + y_by) % Y),
        )
        for s in range(sections)
        for z in range(Z)
        for y in range(Y)
    ]
    return lax.ppermute(array, AXES, pairs)


def from_partner(array):
    return lax.ppermute(array, "tensor", [(0, 1), (1, 0)])


def shape(rows, columns, dtype=BF16):
    return jax.ShapeDtypeStruct((rows, columns), dtype)


def params(limit_mib):
    return pltpu.CompilerParams(vmem_limit_bytes=limit_mib * 1024 * 1024)


def cost(flops, bytes_accessed):
    return pl.CostEstimate(
        flops=int(flops), bytes_accessed=int(bytes_accessed), transcendentals=0
    )


def norm_body(count, *refs):
    parts, gain_ref, (state_ref, out_ref) = refs[:count], refs[count], refs[count + 1 :]
    width = out_ref.shape[1]
    values = parts[0][...].reshape(-1, width).astype(F32)
    for part in parts[1:]:
        values = values + part[...].astype(F32)
    state = values.astype(BF16)
    state_ref[...] = state
    values = state.astype(F32)
    scale = lax.rsqrt(jnp.mean(values * values, axis=-1, keepdims=True) + EPSILON)
    out_ref[...] = (values * scale * gain_ref[...].astype(F32)).astype(BF16)


def norm(parts, gain, index=None):
    rows, width = parts[0].shape[-2:]
    count = len(parts)
    in_specs, extra = [VMEM] * (count + 1), {}
    if index is not None:
        in_specs = [pl.BlockSpec((1, 1, rows, width), lambda i: (index, 0, 0, 0))]
        in_specs.append(pl.BlockSpec((1, width), lambda i: (0, 0)))
        out_spec = pl.BlockSpec((rows, width), lambda i: (0, 0))
        extra = {"grid": (1,)}
    else:
        out_spec = VMEM
    return pl.pallas_call(
        functools.partial(norm_body, count),
        out_shape=[shape(rows, width)] * 2,
        in_specs=in_specs,
        out_specs=[out_spec] * 2,
        compiler_params=params(4),
        cost_estimate=cost(2e8, (count + 2) * rows * width * 2),
        name="norm",
        **extra,
    )(*parts, gain)


def slots_body(pair, capacity, place_ref, router_ref, *refs):
    ids_refs, blocks = refs[:Y], refs[Y : 2 * Y]
    outs, (high_ref, low_ref) = refs[2 * Y : 2 * Y + Z], refs[2 * Y + Z :]
    my_z, my_low, half = place_ref[0], place_ref[1], place_ref[2]
    rows, width = blocks[0].shape
    total = rows * Y
    per = capacity * Y
    experts = router_ref.shape[0]

    logits = jnp.zeros((experts, total), F32)
    for at in range(0, width, 512):
        piece = jnp.concatenate([block[:, at : at + 512] for block in blocks], axis=0)
        logits = logits + lax.dot_general(
            router_ref[:, at : at + 512],
            piece,
            (((1,), (1,)), ((), ())),
            preferred_element_type=F32,
        )

    ids = jnp.concatenate([ref[...] for ref in ids_refs], axis=1)
    first, second = ids[2 * pair : 2 * pair + 1, :], ids[2 * pair + 1 : 2 * pair + 2, :]
    expert = lax.broadcasted_iota(jnp.int32, (experts, total), 0)
    row = lax.broadcasted_iota(jnp.int32, (experts, total), 1)
    at0, at1 = expert == first, expert == second
    named = jnp.where(at0 | at1, 1.0, 0.0).astype(BF16)
    a = lax.broadcasted_iota(jnp.int32, (total, total), 0)
    b = lax.broadcasted_iota(jnp.int32, (total, total), 1)
    earlier = jnp.where((a < b) & (a // rows == b // rows), 1.0, 0.0).astype(BF16)
    position = jnp.dot(named, earlier, preferred_element_type=F32).astype(jnp.int32)
    step = (expert // 2 - my_z + Z) % Z
    block = (row // rows + 2 * half) % Y
    slot = jnp.where(expert % 2 == my_low, step * per + block * capacity + position, -1)
    slot0 = jnp.max(jnp.where(at0, slot, -1), axis=0, keepdims=True)
    slot1 = jnp.max(jnp.where(at1, slot, -1), axis=0, keepdims=True)
    target = lax.broadcasted_iota(jnp.int32, (per * Z, total), 0)
    chosen = jnp.where((target == slot0) | (target == slot1), 1.0, 0.0).astype(BF16)

    @pl.loop(0, width // 512)
    def _(i):
        at = pl.ds(pl.multiple_of(i * 512, 512), 512)
        piece = jnp.concatenate([block[:, at] for block in blocks], axis=0)
        placed = jnp.dot(chosen, piece, preferred_element_type=F32).astype(BF16)
        for k in range(Z):
            outs[k][:, at] = placed[k * per : (k + 1) * per]

    one = jnp.sum(jnp.where(at0, logits, 0.0), axis=0, keepdims=True)
    two = jnp.sum(jnp.where(at1, logits, 0.0), axis=0, keepdims=True)
    weight0 = 1.0 / (1.0 + jnp.exp(two - one))
    weight1 = 1.0 / (1.0 + jnp.exp(one - two))
    spread = jnp.where(target == slot0, weight0, jnp.where(target == slot1, weight1, 0.0))
    high = spread.astype(BF16)
    high_ref[...] = high
    low_ref[...] = (spread - high.astype(F32)).astype(BF16)


def fill_slots(pair, place, router, ids, blocks, capacity):
    rows, width = blocks[0].shape
    per = capacity * Y
    out = pl.pallas_call(
        functools.partial(slots_body, pair, capacity),
        out_shape=[shape(per, width)] * Z + [shape(per * Z, rows * Y)] * 2,
        in_specs=[SMEM, VMEM] + [VMEM] * (2 * Y),
        out_specs=[VMEM] * (Z + 2),
        compiler_params=params(4),
        cost_estimate=cost(1e9, 8 * per * width * 2),
        name="slots",
    )(place, router, *ids, *blocks)
    return out[:Z], out[Z:]


def product_body(count, flip, place_ref, weight_ref, *refs):
    slots, (out_ref, rows_ref) = refs[:count], refs[count:]
    half = place_ref[2]
    if flip:
        half = 1 - half
    units = out_ref.shape[1]
    per = slots[0].shape[0]
    for k in range(count):
        rows_ref[k * per : (k + 1) * per, :] = slots[k][...]

    def columns(at, count):
        here = pl.ds(pl.multiple_of(half * units + at, 128), count)
        part = jnp.dot(rows_ref[...], weight_ref[:, here], preferred_element_type=F32)
        out_ref[:, pl.ds(pl.multiple_of(at, 128), count)] = part.astype(BF16)

    @pl.loop(0, units // CHUNK)
    def _(i):
        columns(i * CHUNK, CHUNK)

    if units % CHUNK:
        columns(units // CHUNK * CHUNK, units % CHUNK)


CHUNK = 768
GROUPS = ((0, 1), (3, 2))


def product(place, combined, slots, flip):
    per, width = slots[0].shape
    count = len(slots)
    units = combined.shape[1] // 2
    return pl.pallas_call(
        functools.partial(product_body, count, flip),
        out_shape=shape(per * count, units),
        in_specs=[SMEM, VMEM] + [VMEM] * count,
        out_specs=VMEM,
        scratch_shapes=[pltpu.VMEM((per * count, width), BF16)],
        compiler_params=params(6),
        cost_estimate=cost(2 * per * count * width * units, width * units * 2),
        name="product_other" if flip else "product_own",
    )(place, combined, *slots)


def down_body(count, offset, place_ref, own_ref, partner_ref, weight_ref, *refs):
    outs, hidden_ref = refs[:count], refs[count]
    first = place_ref[2] == 0
    rows = partner_ref.shape[0]
    width = weight_ref.shape[1]
    band = 80

    @pl.loop(0, rows // band)
    def _(i):
        at = pl.ds(pl.multiple_of(i * band, band), band)
        own_at = pl.ds(pl.multiple_of(offset + i * band, band), band)
        own = own_ref[own_at, :].astype(F32)
        partner = partner_ref[at, :].astype(F32)
        gate = jnp.where(first, own, partner)
        up = jnp.where(first, partner, own)
        hidden_ref[at, :] = (0.5 * gate * (1.0 + jnp.tanh(0.5 * gate)) * up).astype(BF16)

    per = outs[0].shape[0]

    @pl.loop(0, width // 512)
    def _(i):
        at = pl.ds(pl.multiple_of(i * 512, 512), 512)
        part = jnp.dot(hidden_ref[...], weight_ref[:, at], preferred_element_type=F32)
        part = part.astype(BF16)
        for k in range(count):
            outs[k][:, at] = part[k * per : (k + 1) * per]


def down(place, own, partner, weight, count, offset):
    rows, units = partner.shape
    width = weight.shape[1]
    per = rows // count
    return pl.pallas_call(
        functools.partial(down_body, count, offset),
        out_shape=[shape(per, width)] * count,
        in_specs=[SMEM, VMEM, VMEM, VMEM],
        out_specs=[VMEM] * count,
        scratch_shapes=[pltpu.VMEM((rows, units), BF16)],
        compiler_params=params(6),
        cost_estimate=cost(2 * rows * width * units, width * units * 2),
        name="down",
    )(place, own, partner, weight)


def collect_body(state_ref, high_ref, low_ref, *refs):
    returned, outs = refs[:Z], refs[Z:]
    rows, width = outs[0].shape

    def weighted(weights, piece):
        return lax.dot_general(
            weights, piece, (((0,), (0,)), ((), ())), preferred_element_type=F32
        )

    @pl.loop(0, width // 512)
    def _(i):
        at = pl.ds(pl.multiple_of(i * 512, 512), 512)
        piece = jnp.concatenate([part[:, at] for part in returned], axis=0)
        total = weighted(high_ref[...], piece) + weighted(low_ref[...], piece)
        own = state_ref[:, at].astype(F32) + total[:rows]
        outs[0][:, at] = own.astype(BF16)
        for j in range(1, Y):
            outs[j][:, at] = total[j * rows : (j + 1) * rows].astype(BF16)


def collect(state, high, low, returned):
    rows = high.shape[1] // Y
    width = returned[0].shape[1]
    return pl.pallas_call(
        collect_body,
        out_shape=[shape(rows, width)] * Y,
        in_specs=[VMEM] * (3 + Z),
        out_specs=[VMEM] * Y,
        compiler_params=params(6),
        cost_estimate=cost(1e9, 4e6),
        name="collect",
    )(state, high, low, *returned)


def on_device(tokens, norm_gain, router_weight, gate_up, down_proj, expert_ids):
    experts = router_weight.shape[2]
    rows = tokens.shape[2]
    capacity = rows * 2 * 5 // (4 * experts)
    expert_index = lax.axis_index("expert")
    place = jnp.stack([expert_index // 2, expert_index % 2, lax.axis_index("tensor")]).astype(
        jnp.int32
    )
    combined, down_rows = gate_up[0, 0], down_proj[0, 0]

    router = router_weight[0].T
    ids = expert_ids[:, :, 0].transpose(0, 1, 3, 2).reshape(-1, rows)
    normed_first = [norm([tokens], norm_gain, m) for m in (0, 1)]
    ids, normed_first[1] = lax.optimization_barrier((ids, normed_first[1]))
    ids = [ids] + [y_shift(ids, j) for j in range(1, Y)]

    parts = None
    for tick in range(TICKS):
        streams = []
        for m in (0, 1):
            to_next = 1 if m == 0 else -1
            state, normed = normed_first[m] if tick == 0 else norm(parts[m], norm_gain)
            blocks = [normed] + [y_shift(normed, j) for j in range(1, Y)]
            slots, (high, low) = fill_slots(2 * tick + m, place, router, ids, blocks, capacity)
            arrived = [slots[0]] + [z_shift(slots[k], k) for k in range(1, Z)]
            returned = [None] * Z
            partners = [
                from_partner(product(place, combined, [arrived[k] for k in group], True))
                for group in GROUPS
            ]
            order = [k for group in GROUPS for k in group]
            own = product(place, combined, [arrived[k] for k in order], False)
            offset = 0
            for group, partner in zip(GROUPS, partners):
                back = down(place, own, partner, down_rows, len(group), offset)
                offset += partner.shape[0]
                for k, piece in zip(group, back):
                    returned[k] = z_shift(piece, -k) if k else piece
            sums = collect(state, high, low, returned)
            streams.append([section_shift(sums[j], to_next, -j) for j in range(Y)])
        parts = streams
    total = [sum(piece.astype(F32) for piece in stream).astype(BF16) for stream in parts]
    return jnp.stack(total)[:, None]


def solution(mesh):
    in_specs = (
        P(None, "section", ("expert", "tensor"), None),
        P("section", None),
        P("section", None, None),
        P("section", "expert", None, "tensor"),
        P("section", "expert", "tensor", None),
        P(None, None, "section", ("expert", "tensor"), None),
    )
    out_specs = P(None, "section", ("expert", "tensor"), None)
    return jax.shard_map(
        on_device, mesh=mesh, in_specs=in_specs, out_specs=out_specs, check_vma=False
    )
```

```python
import functools

import jax
import jax.numpy as jnp
from jax import lax
from jax.experimental import pallas as pl
from jax.experimental.pallas import tpu as pltpu
from jax.sharding import PartitionSpec as P

TICKS = 2
EPSILON = 1e-05

BF16 = jnp.bfloat16
F32 = jnp.float32
VMEM = pl.BlockSpec(memory_space=pltpu.VMEM)
SMEM = pl.BlockSpec(memory_space=pltpu.SMEM)

Z = 4
Y = 4
AXES = ("section", "expert", "tensor")
PLANE = ("expert", "tensor")


def plane_index(z, y):
    return (z * 2 + y % 2) * 2 + y // 2


def y_shift(array, by):
    pairs = [
        (plane_index(z, y), plane_index(z, (y + by) % Y)) for z in range(Z) for y in range(Y)
    ]
    return lax.ppermute(array, PLANE, pairs)


def z_shift(array, by):
    pairs = [
        (plane_index(z, y), plane_index((z + by) % Z, y)) for z in range(Z) for y in range(Y)
    ]
    return lax.ppermute(array, PLANE, pairs)


def section_shift(array, by, y_by):
    sections = lax.axis_size("section")
    plane = Z * Y
    pairs = [
        (
            s * plane + plane_index(z, y),
            (s + by) % sections * plane + plane_index(z, (y + y_by) % Y),
        )
        for s in range(sections)
        for z in range(Z)
        for y in range(Y)
    ]
    return lax.ppermute(array, AXES, pairs)


def from_partner(array):
    return lax.ppermute(array, "tensor", [(0, 1), (1, 0)])


def shape(rows, columns, dtype=BF16):
    return jax.ShapeDtypeStruct((rows, columns), dtype)


def params(limit_mib):
    return pltpu.CompilerParams(vmem_limit_bytes=limit_mib * 1024 * 1024)


def cost(flops, bytes_accessed):
    return pl.CostEstimate(
        flops=int(flops), bytes_accessed=int(bytes_accessed), transcendentals=0
    )


def norm_body(count, *refs):
    parts, gain_ref, (state_ref, out_ref) = refs[:count], refs[count], refs[count + 1 :]
    width = out_ref.shape[1]
    values = parts[0][...].reshape(-1, width).astype(F32)
    for part in parts[1:]:
        values = values + part[...].astype(F32)
    state = values.astype(BF16)
    state_ref[...] = state
    values = state.astype(F32)
    scale = lax.rsqrt(jnp.mean(values * values, axis=-1, keepdims=True) + EPSILON)
    out_ref[...] = (values * scale * gain_ref[...].astype(F32)).astype(BF16)


def norm(parts, gain, index=None):
    rows, width = parts[0].shape[-2:]
    count = len(parts)
    in_specs, extra = [VMEM] * (count + 1), {}
    if index is not None:
        in_specs = [pl.BlockSpec((1, 1, rows, width), lambda i: (index, 0, 0, 0))]
        in_specs.append(pl.BlockSpec((1, width), lambda i: (0, 0)))
        out_spec = pl.BlockSpec((rows, width), lambda i: (0, 0))
        extra = {"grid": (1,)}
    else:
        out_spec = VMEM
    return pl.pallas_call(
        functools.partial(norm_body, count),
        out_shape=[shape(rows, width)] * 2,
        in_specs=in_specs,
        out_specs=[out_spec] * 2,
        compiler_params=params(4),
        cost_estimate=cost(2e8, (count + 2) * rows * width * 2),
        name="norm",
        **extra,
    )(*parts, gain)


def slots_body(pair, capacity, place_ref, router_ref, *refs):
    ids_refs, blocks = refs[:Y], refs[Y : 2 * Y]
    outs, (high_ref, low_ref) = refs[2 * Y : 2 * Y + Z], refs[2 * Y + Z :]
    my_z, my_low, half = place_ref[0], place_ref[1], place_ref[2]
    rows, width = blocks[0].shape
    total = rows * Y
    per = capacity * Y
    experts = router_ref.shape[0]

    logits = jnp.zeros((experts, total), F32)
    for at in range(0, width, 512):
        piece = jnp.concatenate([block[:, at : at + 512] for block in blocks], axis=0)
        logits = logits + lax.dot_general(
            router_ref[:, at : at + 512],
            piece,
            (((1,), (1,)), ((), ())),
            preferred_element_type=F32,
        )

    ids = jnp.concatenate([ref[...] for ref in ids_refs], axis=1)
    first, second = ids[2 * pair : 2 * pair + 1, :], ids[2 * pair + 1 : 2 * pair + 2, :]
    expert = lax.broadcasted_iota(jnp.int32, (experts, total), 0)
    row = lax.broadcasted_iota(jnp.int32, (experts, total), 1)
    at0, at1 = expert == first, expert == second
    named = jnp.where(at0 | at1, 1.0, 0.0).astype(BF16)
    a = lax.broadcasted_iota(jnp.int32, (total, total), 0)
    b = lax.broadcasted_iota(jnp.int32, (total, total), 1)
    earlier = jnp.where((a < b) & (a // rows == b // rows), 1.0, 0.0).astype(BF16)
    position = jnp.dot(named, earlier, preferred_element_type=F32).astype(jnp.int32)
    step = (expert // 2 - my_z + Z) % Z
    block = (row // rows + 2 * half) % Y
    slot = jnp.where(expert % 2 == my_low, step * per + block * capacity + position, -1)
    slot0 = jnp.max(jnp.where(at0, slot, -1), axis=0, keepdims=True)
    slot1 = jnp.max(jnp.where(at1, slot, -1), axis=0, keepdims=True)
    target = lax.broadcasted_iota(jnp.int32, (per * Z, total), 0)
    chosen = jnp.where((target == slot0) | (target == slot1), 1.0, 0.0).astype(BF16)

    @pl.loop(0, width // 512)
    def _(i):
        at = pl.ds(pl.multiple_of(i * 512, 512), 512)
        piece = jnp.concatenate([block[:, at] for block in blocks], axis=0)
        placed = jnp.dot(chosen, piece, preferred_element_type=F32).astype(BF16)
        for k in range(Z):
            outs[k][:, at] = placed[k * per : (k + 1) * per]

    one = jnp.sum(jnp.where(at0, logits, 0.0), axis=0, keepdims=True)
    two = jnp.sum(jnp.where(at1, logits, 0.0), axis=0, keepdims=True)
    weight0 = 1.0 / (1.0 + jnp.exp(two - one))
    weight1 = 1.0 / (1.0 + jnp.exp(one - two))
    spread = jnp.where(target == slot0, weight0, jnp.where(target == slot1, weight1, 0.0))
    high = spread.astype(BF16)
    high_ref[...] = high
    low_ref[...] = (spread - high.astype(F32)).astype(BF16)


def fill_slots(pair, place, router, ids, blocks, capacity):
    rows, width = blocks[0].shape
    per = capacity * Y
    out = pl.pallas_call(
        functools.partial(slots_body, pair, capacity),
        out_shape=[shape(per, width)] * Z + [shape(per * Z, rows * Y)] * 2,
        in_specs=[SMEM, VMEM] + [VMEM] * (2 * Y),
        out_specs=[VMEM] * (Z + 2),
        compiler_params=params(4),
        cost_estimate=cost(1e9, 8 * per * width * 2),
        name="slots",
    )(place, router, *ids, *blocks)
    return out[:Z], out[Z:]


def product_body(count, flip, place_ref, weight_ref, *refs):
    slots, (out_ref, rows_ref) = refs[:count], refs[count:]
    half = place_ref[2]
    if flip:
        half = 1 - half
    units = out_ref.shape[1]
    per = slots[0].shape[0]
    for k in range(count):
        rows_ref[k * per : (k + 1) * per, :] = slots[k][...]

    @pl.loop(0, pl.cdiv(units, CHUNK))
    def _(i):
        at = pl.multiple_of(jnp.minimum(i * CHUNK, units - CHUNK), 128)
        here = pl.ds(pl.multiple_of(half * units + at, 128), CHUNK)
        part = jnp.dot(rows_ref[...], weight_ref[:, here], preferred_element_type=F32)
        out_ref[:, pl.ds(at, CHUNK)] = part.astype(BF16)


CHUNK = 512
GROUPS = ((0, 1), (3, 2))


def product(place, combined, slots, flip):
    per, width = slots[0].shape
    count = len(slots)
    units = combined.shape[1] // 2
    return pl.pallas_call(
        functools.partial(product_body, count, flip),
        out_shape=shape(per * count, units),
        in_specs=[SMEM, VMEM] + [VMEM] * count,
        out_specs=VMEM,
        scratch_shapes=[pltpu.VMEM((per * count, width), BF16)],
        compiler_params=params(6),
        cost_estimate=cost(2 * per * count * width * units, width * units * 2),
        name="product_other" if flip else "product_own",
    )(place, combined, *slots)


def down_body(count, offset, place_ref, own_ref, partner_ref, weight_ref, *refs):
    outs, hidden_ref = refs[:count], refs[count]
    first = place_ref[2] == 0
    rows = partner_ref.shape[0]
    width = weight_ref.shape[1]
    band = 80

    @pl.loop(0, rows // band)
    def _(i):
        at = pl.ds(pl.multiple_of(i * band, band), band)
        own_at = pl.ds(pl.multiple_of(offset + i * band, band), band)
        own = own_ref[own_at, :].astype(F32)
        partner = partner_ref[at, :].astype(F32)
        gate = jnp.where(first, own, partner)
        up = jnp.where(first, partner, own)
        hidden_ref[at, :] = (0.5 * gate * (1.0 + jnp.tanh(0.5 * gate)) * up).astype(BF16)

    per = outs[0].shape[0]

    @pl.loop(0, width // 512)
    def _(i):
        at = pl.ds(pl.multiple_of(i * 512, 512), 512)
        part = jnp.dot(hidden_ref[...], weight_ref[:, at], preferred_element_type=F32)
        part = part.astype(BF16)
        for k in range(count):
            outs[k][:, at] = part[k * per : (k + 1) * per]


def down(place, own, partner, weight, count, offset):
    rows, units = partner.shape
    width = weight.shape[1]
    per = rows // count
    return pl.pallas_call(
        functools.partial(down_body, count, offset),
        out_shape=[shape(per, width)] * count,
        in_specs=[SMEM, VMEM, VMEM, VMEM],
        out_specs=[VMEM] * count,
        scratch_shapes=[pltpu.VMEM((rows, units), BF16)],
        compiler_params=params(6),
        cost_estimate=cost(2 * rows * width * units, width * units * 2),
        name="down",
    )(place, own, partner, weight)


def collect_body(state_ref, high_ref, low_ref, *refs):
    returned, outs = refs[:Z], refs[Z:]
    rows, width = outs[0].shape

    def weighted(weights, piece):
        return lax.dot_general(
            weights, piece, (((0,), (0,)), ((), ())), preferred_element_type=F32
        )

    @pl.loop(0, width // 512)
    def _(i):
        at = pl.ds(pl.multiple_of(i * 512, 512), 512)
        piece = jnp.concatenate([part[:, at] for part in returned], axis=0)
        total = weighted(high_ref[...], piece) + weighted(low_ref[...], piece)
        own = state_ref[:, at].astype(F32) + total[:rows]
        outs[0][:, at] = own.astype(BF16)
        for j in range(1, Y):
            outs[j][:, at] = total[j * rows : (j + 1) * rows].astype(BF16)


def collect(state, high, low, returned):
    rows = high.shape[1] // Y
    width = returned[0].shape[1]
    return pl.pallas_call(
        collect_body,
        out_shape=[shape(rows, width)] * Y,
        in_specs=[VMEM] * (3 + Z),
        out_specs=[VMEM] * Y,
        compiler_params=params(6),
        cost_estimate=cost(1e9, 4e6),
        name="collect",
    )(state, high, low, *returned)


def on_device(tokens, norm_gain, router_weight, gate_up, down_proj, expert_ids):
    experts = router_weight.shape[2]
    rows = tokens.shape[2]
    capacity = rows * 2 * 5 // (4 * experts)
    expert_index = lax.axis_index("expert")
    place = jnp.stack([expert_index // 2, expert_index % 2, lax.axis_index("tensor")]).astype(
        jnp.int32
    )
    combined, down_rows = gate_up[0, 0], down_proj[0, 0]

    router = router_weight[0].T
    ids = expert_ids[:, :, 0].transpose(0, 1, 3, 2).reshape(-1, rows)
    normed_first = [norm([tokens], norm_gain, m) for m in (0, 1)]
    ids, normed_first[1] = lax.optimization_barrier((ids, normed_first[1]))
    ids = [ids] + [y_shift(ids, j) for j in range(1, Y)]

    parts = None
    for tick in range(TICKS):
        streams = []
        for m in (0, 1):
            to_next = 1 if m == 0 else -1
            state, normed = normed_first[m] if tick == 0 else norm(parts[m], norm_gain)
            blocks = [normed] + [y_shift(normed, j) for j in range(1, Y)]
            slots, (high, low) = fill_slots(2 * tick + m, place, router, ids, blocks, capacity)
            arrived = [slots[0]] + [z_shift(slots[k], k) for k in range(1, Z)]
            returned = [None] * Z
            partners = [
                from_partner(product(place, combined, [arrived[k] for k in group], True))
                for group in GROUPS
            ]
            order = [k for group in GROUPS for k in group]
            own = product(place, combined, [arrived[k] for k in order], False)
            offset = 0
            for group, partner in zip(GROUPS, partners):
                back = down(place, own, partner, down_rows, len(group), offset)
                offset += partner.shape[0]
                for k, piece in zip(group, back):
                    returned[k] = z_shift(piece, -k) if k else piece
            sums = collect(state, high, low, returned)
            streams.append([section_shift(sums[j], to_next, -j) for j in range(Y)])
        parts = streams
    total = [sum(piece.astype(F32) for piece in stream).astype(BF16) for stream in parts]
    return jnp.stack(total)[:, None]


def solution(mesh):
    in_specs = (
        P(None, "section", ("expert", "tensor"), None),
        P("section", None),
        P("section", None, None),
        P("section", "expert", None, "tensor"),
        P("section", "expert", "tensor", None),
        P(None, None, "section", ("expert", "tensor"), None),
    )
    out_specs = P(None, "section", ("expert", "tensor"), None)
    return jax.shard_map(
        on_device, mesh=mesh, in_specs=in_specs, out_specs=out_specs, check_vma=False
    )
```

```python
import functools

import jax
import jax.numpy as jnp
from jax import lax
from jax.experimental import pallas as pl
from jax.experimental.pallas import tpu as pltpu
from jax.sharding import PartitionSpec as P

TICKS = 2
EPSILON = 1e-05

BF16 = jnp.bfloat16
F32 = jnp.float32
VMEM = pl.BlockSpec(memory_space=pltpu.VMEM)
SMEM = pl.BlockSpec(memory_space=pltpu.SMEM)

Z = 4
Y = 4
AXES = ("section", "expert", "tensor")
PLANE = ("expert", "tensor")


def plane_index(z, y):
    return (z * 2 + y % 2) * 2 + y // 2


def y_shift(array, by):
    pairs = [
        (plane_index(z, y), plane_index(z, (y + by) % Y)) for z in range(Z) for y in range(Y)
    ]
    return lax.ppermute(array, PLANE, pairs)


def z_shift(array, by):
    pairs = [
        (plane_index(z, y), plane_index((z + by) % Z, y)) for z in range(Z) for y in range(Y)
    ]
    return lax.ppermute(array, PLANE, pairs)


def section_shift(array, by, y_by):
    sections = lax.axis_size("section")
    plane = Z * Y
    pairs = [
        (
            s * plane + plane_index(z, y),
            (s + by) % sections * plane + plane_index(z, (y + y_by) % Y),
        )
        for s in range(sections)
        for z in range(Z)
        for y in range(Y)
    ]
    return lax.ppermute(array, AXES, pairs)


def from_partner(array):
    return lax.ppermute(array, "tensor", [(0, 1), (1, 0)])


def shape(rows, columns, dtype=BF16):
    return jax.ShapeDtypeStruct((rows, columns), dtype)


def params(limit_mib):
    return pltpu.CompilerParams(vmem_limit_bytes=limit_mib * 1024 * 1024)


def cost(flops, bytes_accessed):
    return pl.CostEstimate(
        flops=int(flops), bytes_accessed=int(bytes_accessed), transcendentals=0
    )


def norm_body(count, *refs):
    parts, gain_ref, (state_ref, out_ref) = refs[:count], refs[count], refs[count + 1 :]
    width = out_ref.shape[1]
    values = parts[0][...].reshape(-1, width).astype(F32)
    for part in parts[1:]:
        values = values + part[...].astype(F32)
    state = values.astype(BF16)
    state_ref[...] = state
    values = state.astype(F32)
    scale = lax.rsqrt(jnp.mean(values * values, axis=-1, keepdims=True) + EPSILON)
    out_ref[...] = (values * scale * gain_ref[...].astype(F32)).astype(BF16)


def norm(parts, gain, index=None):
    rows, width = parts[0].shape[-2:]
    count = len(parts)
    in_specs, extra = [VMEM] * (count + 1), {}
    if index is not None:
        in_specs = [pl.BlockSpec((1, 1, rows, width), lambda i: (index, 0, 0, 0))]
        in_specs.append(pl.BlockSpec((1, width), lambda i: (0, 0)))
        out_spec = pl.BlockSpec((rows, width), lambda i: (0, 0))
        extra = {"grid": (1,)}
    else:
        out_spec = VMEM
    return pl.pallas_call(
        functools.partial(norm_body, count),
        out_shape=[shape(rows, width)] * 2,
        in_specs=in_specs,
        out_specs=[out_spec] * 2,
        compiler_params=params(4),
        cost_estimate=cost(2e8, (count + 2) * rows * width * 2),
        name="norm",
        **extra,
    )(*parts, gain)


def slots_body(pair, capacity, place_ref, router_ref, *refs):
    ids_refs, blocks = refs[:Y], refs[Y : 2 * Y]
    outs, (high_ref, low_ref) = refs[2 * Y : 2 * Y + Z], refs[2 * Y + Z :]
    my_z, my_low, half = place_ref[0], place_ref[1], place_ref[2]
    rows, width = blocks[0].shape
    total = rows * Y
    per = capacity * Y
    experts = router_ref.shape[0]

    logits = jnp.zeros((experts, total), F32)
    for at in range(0, width, 512):
        piece = jnp.concatenate([block[:, at : at + 512] for block in blocks], axis=0)
        logits = logits + lax.dot_general(
            router_ref[:, at : at + 512],
            piece,
            (((1,), (1,)), ((), ())),
            preferred_element_type=F32,
        )

    ids = jnp.concatenate([ref[...] for ref in ids_refs], axis=1)
    first, second = ids[2 * pair : 2 * pair + 1, :], ids[2 * pair + 1 : 2 * pair + 2, :]
    expert = lax.broadcasted_iota(jnp.int32, (experts, total), 0)
    row = lax.broadcasted_iota(jnp.int32, (experts, total), 1)
    at0, at1 = expert == first, expert == second
    named = jnp.where(at0 | at1, 1.0, 0.0).astype(BF16)
    a = lax.broadcasted_iota(jnp.int32, (total, total), 0)
    b = lax.broadcasted_iota(jnp.int32, (total, total), 1)
    earlier = jnp.where((a < b) & (a // rows == b // rows), 1.0, 0.0).astype(BF16)
    position = jnp.dot(named, earlier, preferred_element_type=F32).astype(jnp.int32)
    step = (expert // 2 - my_z + Z) % Z
    block = (row // rows + 2 * half) % Y
    slot = jnp.where(expert % 2 == my_low, step * per + block * capacity + position, -1)
    slot0 = jnp.max(jnp.where(at0, slot, -1), axis=0, keepdims=True)
    slot1 = jnp.max(jnp.where(at1, slot, -1), axis=0, keepdims=True)
    target = lax.broadcasted_iota(jnp.int32, (per * Z, total), 0)
    chosen = jnp.where((target == slot0) | (target == slot1), 1.0, 0.0).astype(BF16)

    @pl.loop(0, width // 512)
    def _(i):
        at = pl.ds(pl.multiple_of(i * 512, 512), 512)
        piece = jnp.concatenate([block[:, at] for block in blocks], axis=0)
        placed = jnp.dot(chosen, piece, preferred_element_type=F32).astype(BF16)
        for k in range(Z):
            outs[k][:, at] = placed[k * per : (k + 1) * per]

    one = jnp.sum(jnp.where(at0, logits, 0.0), axis=0, keepdims=True)
    two = jnp.sum(jnp.where(at1, logits, 0.0), axis=0, keepdims=True)
    weight0 = 1.0 / (1.0 + jnp.exp(two - one))
    weight1 = 1.0 / (1.0 + jnp.exp(one - two))
    spread = jnp.where(target == slot0, weight0, jnp.where(target == slot1, weight1, 0.0))
    high = spread.astype(BF16)
    high_ref[...] = high
    low_ref[...] = (spread - high.astype(F32)).astype(BF16)


def fill_slots(pair, place, router, ids, blocks, capacity):
    rows, width = blocks[0].shape
    per = capacity * Y
    out = pl.pallas_call(
        functools.partial(slots_body, pair, capacity),
        out_shape=[shape(per, width)] * Z + [shape(per * Z, rows * Y)] * 2,
        in_specs=[SMEM, VMEM] + [VMEM] * (2 * Y),
        out_specs=[VMEM] * (Z + 2),
        compiler_params=params(4),
        cost_estimate=cost(1e9, 8 * per * width * 2),
        name="slots",
    )(place, router, *ids, *blocks)
    return out[:Z], out[Z:]


def product_body(count, flip, place_ref, weight_ref, *refs):
    slots, (out_ref, rows_ref) = refs[:count], refs[count:]
    half = place_ref[2]
    if flip:
        half = 1 - half
    units = out_ref.shape[1]
    per = slots[0].shape[0]
    for k in range(count):
        rows_ref[k * per : (k + 1) * per, :] = slots[k][...]

    @pl.loop(0, pl.cdiv(units, CHUNK))
    def _(i):
        at = pl.multiple_of(jnp.minimum(i * CHUNK, units - CHUNK), 128)
        here = pl.ds(pl.multiple_of(half * units + at, 128), CHUNK)
        part = jnp.dot(rows_ref[...], weight_ref[:, here], preferred_element_type=F32)
        out_ref[:, pl.ds(at, CHUNK)] = part.astype(BF16)


CHUNK = 512
GROUPS = ((0, 1), (3, 2))


def product(place, combined, slots, flip):
    per, width = slots[0].shape
    count = len(slots)
    units = combined.shape[1] // 2
    return pl.pallas_call(
        functools.partial(product_body, count, flip),
        out_shape=shape(per * count, units),
        in_specs=[SMEM, VMEM] + [VMEM] * count,
        out_specs=VMEM,
        scratch_shapes=[pltpu.VMEM((per * count, width), BF16)],
        compiler_params=params(6),
        cost_estimate=cost(2 * per * count * width * units, width * units * 2),
        name="product_other" if flip else "product_own",
    )(place, combined, *slots)


def down_body(count, offset, place_ref, own_ref, partner_ref, weight_ref, *refs):
    outs, hidden_ref = refs[:count], refs[count]
    first = place_ref[2] == 0
    rows = partner_ref.shape[0]
    width = weight_ref.shape[1]
    band = 80

    @pl.loop(0, rows // band)
    def _(i):
        at = pl.ds(pl.multiple_of(i * band, band), band)
        own_at = pl.ds(pl.multiple_of(offset + i * band, band), band)
        own = own_ref[own_at, :].astype(F32)
        partner = partner_ref[at, :].astype(F32)
        gate = jnp.where(first, own, partner)
        up = jnp.where(first, partner, own)
        hidden_ref[at, :] = (0.5 * gate * (1.0 + jnp.tanh(0.5 * gate)) * up).astype(BF16)

    per = outs[0].shape[0]

    @pl.loop(0, width // 1024)
    def _(i):
        at = pl.ds(pl.multiple_of(i * 1024, 1024), 1024)
        part = jnp.dot(hidden_ref[...], weight_ref[:, at], preferred_element_type=F32)
        part = part.astype(BF16)
        for k in range(count):
            outs[k][:, at] = part[k * per : (k + 1) * per]


def down(place, own, partner, weight, count, offset):
    rows, units = partner.shape
    width = weight.shape[1]
    per = rows // count
    return pl.pallas_call(
        functools.partial(down_body, count, offset),
        out_shape=[shape(per, width)] * count,
        in_specs=[SMEM, VMEM, VMEM, VMEM],
        out_specs=[VMEM] * count,
        scratch_shapes=[pltpu.VMEM((rows, units), BF16)],
        compiler_params=params(6),
        cost_estimate=cost(2 * rows * width * units, width * units * 2),
        name="down",
    )(place, own, partner, weight)


def collect_body(state_ref, high_ref, low_ref, *refs):
    returned, outs = refs[:Z], refs[Z:]
    rows, width = outs[0].shape

    def weighted(weights, piece):
        return lax.dot_general(
            weights, piece, (((0,), (0,)), ((), ())), preferred_element_type=F32
        )

    @pl.loop(0, width // 512)
    def _(i):
        at = pl.ds(pl.multiple_of(i * 512, 512), 512)
        piece = jnp.concatenate([part[:, at] for part in returned], axis=0)
        total = weighted(high_ref[...], piece) + weighted(low_ref[...], piece)
        own = state_ref[:, at].astype(F32) + total[:rows]
        outs[0][:, at] = own.astype(BF16)
        for j in range(1, Y):
            outs[j][:, at] = total[j * rows : (j + 1) * rows].astype(BF16)


def collect(state, high, low, returned):
    rows = high.shape[1] // Y
    width = returned[0].shape[1]
    return pl.pallas_call(
        collect_body,
        out_shape=[shape(rows, width)] * Y,
        in_specs=[VMEM] * (3 + Z),
        out_specs=[VMEM] * Y,
        compiler_params=params(6),
        cost_estimate=cost(1e9, 4e6),
        name="collect",
    )(state, high, low, *returned)


def on_device(tokens, norm_gain, router_weight, gate_up, down_proj, expert_ids):
    experts = router_weight.shape[2]
    rows = tokens.shape[2]
    capacity = rows * 2 * 5 // (4 * experts)
    expert_index = lax.axis_index("expert")
    place = jnp.stack([expert_index // 2, expert_index % 2, lax.axis_index("tensor")]).astype(
        jnp.int32
    )
    combined, down_rows = gate_up[0, 0], down_proj[0, 0]

    router = router_weight[0].T
    ids = expert_ids[:, :, 0].transpose(0, 1, 3, 2).reshape(-1, rows)
    normed_first = [norm([tokens], norm_gain, m) for m in (0, 1)]
    ids, normed_first[1] = lax.optimization_barrier((ids, normed_first[1]))
    ids = [ids] + [y_shift(ids, j) for j in range(1, Y)]

    parts = None
    for tick in range(TICKS):
        streams = []
        for m in (0, 1):
            to_next = 1 if m == 0 else -1
            state, normed = normed_first[m] if tick == 0 else norm(parts[m], norm_gain)
            blocks = [normed] + [y_shift(normed, j) for j in range(1, Y)]
            slots, (high, low) = fill_slots(2 * tick + m, place, router, ids, blocks, capacity)
            arrived = [slots[0]] + [z_shift(slots[k], k) for k in range(1, Z)]
            returned = [None] * Z
            partners = [
                from_partner(product(place, combined, [arrived[k] for k in group], True))
                for group in GROUPS
            ]
            order = [k for group in GROUPS for k in group]
            own = product(place, combined, [arrived[k] for k in order], False)
            offset = 0
            for group, partner in zip(GROUPS, partners):
                back = down(place, own, partner, down_rows, len(group), offset)
                offset += partner.shape[0]
                for k, piece in zip(group, back):
                    returned[k] = z_shift(piece, -k) if k else piece
            sums = collect(state, high, low, returned)
            streams.append([section_shift(sums[j], to_next, -j) for j in (2, 1, 3, 0)])
        parts = streams
    total = [sum(piece.astype(F32) for piece in stream).astype(BF16) for stream in parts]
    return jnp.stack(total)[:, None]


def solution(mesh):
    in_specs = (
        P(None, "section", ("expert", "tensor"), None),
        P("section", None),
        P("section", None, None),
        P("section", "expert", None, "tensor"),
        P("section", "expert", "tensor", None),
        P(None, None, "section", ("expert", "tensor"), None),
    )
    out_specs = P(None, "section", ("expert", "tensor"), None)
    return jax.shard_map(
        on_device, mesh=mesh, in_specs=in_specs, out_specs=out_specs, check_vma=False
    )
```
